32 devices in a mesh: dp: 8 (over y, x, core), expert: 4 (over z).
Axes of the slice: x: 2, y: 2, z: 4, core: 2. Of those that a mesh axis runs over, the one named last changes fastest.
Arguments:
- hidden_act: bfloat16 [4096, 2048], P('dp', 'expert'), may hold values from -6 to 6
- out_grad: bfloat16 [4096, 7168], P('dp'), may hold values from -0.125 to 0.125
- counts: int32 [8], P('dp'), may hold values from 0 to 512
- expert_master: float32 [7168, 2048], P('dp', 'expert'), may hold values from -0.005 to 0.005
- expert_mom: float32 [7168, 2048], P('dp', 'expert'), may hold values from -0.12 to 0.12
- expert_var: float32 [7168, 2048], P('dp', 'expert'), may hold values from 0.001 to 0.1
- dense_partial: float32 [8, 4, 14336], P('dp', 'expert'), may hold values from -0.8 to 0.8
- dense_master: float32 [14336], replicated, may hold values from 0.5 to 1.5
- dense_mom: float32 [14336], replicated, may hold values from -2 to 2
- dense_var: float32 [14336], replicated, may hold values from 0.1 to 10
Outputs:
- routed_weight: bfloat16 [7168, 2048], P(None, 'expert')
- new_expert_master: float32 [7168, 2048], P('dp', 'expert')
- new_expert_mom: float32 [7168, 2048], P('dp', 'expert')
- new_expert_var: float32 [7168, 2048], P('dp', 'expert')
- new_dense_master: float32 [14336], replicated
- new_dense_mom: float32 [14336], replicated
- new_dense_var: float32 [14336], replicated
The draws below stay inside these ranges and needn't reach their ends.
All inputs are finite; a program needn't handle non-finite values.
Results may differ from the reference program's by a relative error of at most 0.0004.
Values may be sent and summed in bfloat16 or wider, within the bound.
No kernel may reach another device: no remote copies, remote signals or barrier semaphores. Data moves between devices by JAX's collectives and lax.ppermute only.
A program may use at most 128 MiB of HBM per device.

```python
import math
import jax
import jax.numpy as jnp
from jax import lax

D = 7168
FFE = 2048
CAP = 512
ROWS = 4096
GAINS = 14336
N_DP = 8
N_EXPERT = 4


def plant(drawn, key, least, top_value):
    shape = drawn.shape
    index_at = [jax.random.randint(jax.random.fold_in(key, axis), (), 0, shape[axis]) for axis in range(len(shape))]
    drawn = drawn.at[tuple(index_at)].set(least)
    longest = shape.index(max(shape))
    index_at[longest] = (index_at[longest] + 1) % shape[longest]
    return drawn.at[tuple(index_at)].set(top_value)


def with_spikes(result, key, source, target, blocks, factor):
    def block_of(position):
        return (jnp.arange(result.shape[position]) // (result.shape[position] // blocks)).reshape((-1,) + (1,) * (result.ndim - 1 - position))

    one_side = jax.random.permutation(key, blocks)[block_of(target)]
    other_side = (block_of(target) + blocks // 2) % blocks
    return jnp.where((block_of(source) == one_side) | (block_of(source) == other_side), factor * result, result)


def shard_levels(stream_key, dims, cuts, low, top_value):
    def one(position, parts):
        draws = jax.random.uniform(jax.random.fold_in(jax.random.fold_in(stream_key, 6), position), (parts,), jnp.float32, low / len(cuts), top_value / len(cuts))
        return jnp.repeat(jnp.exp(draws), dims[position] // parts).reshape((-1,) + (1,) * (len(dims) - position - 1))

    loudness = one(*cuts[0])
    for cut in cuts[1:]:
        loudness = loudness * one(*cut)
    return loudness


def scatter_about(stream_key, shape, deviation, reach, split=(), kind=jnp.bfloat16):
    gain = shard_levels(stream_key, shape, split, -0.22, 0.18) if split else 1.0
    drawn = jax.random.normal(stream_key, shape, jnp.float32) * deviation * gain
    return jnp.minimum(jnp.maximum(drawn, -reach), reach).astype(kind)


def heavy_noise(own_key, shape, scale, limit, pieces, heavy, held_as=jnp.bfloat16):
    result = scale * jax.random.normal(own_key, shape, jnp.float32)
    if pieces:
        result = result * shard_levels(own_key, shape, pieces, -0.22, 0.18)
    return jnp.clip(with_spikes(result, jax.random.fold_in(own_key, 3), *heavy), -limit, limit).astype(held_as)


def setup_inputs(seed: int = 0) -> dict:
    keys = jax.random.split(jax.random.key(seed), 11)
    hidden_act = scatter_about(keys[0], (ROWS, FFE), 1.0, 6.0, ((0, 8), (1, 4)))
    out_grad = heavy_noise(keys[1], (ROWS, D), ROWS ** -0.5, 0.125, ((0, 8),), (0, 1, 8, 2.0))
    counts = plant(jax.random.randint(keys[2], (N_DP,), 0, CAP + 1), jax.random.fold_in(keys[2], 1), 0, CAP).astype(jnp.int32)
    expert_master = scatter_about(keys[3], (D, FFE), 0.0008, 0.005, ((0, 8), (1, 4)), jnp.float32)
    expert_mom = scatter_about(keys[4], (D, FFE), 0.02, 0.12, ((0, 8), (1, 4)), jnp.float32)
    expert_var = jnp.clip(jnp.exp(math.log(0.1) - 4.6051702 * jax.random.uniform(keys[5], (D, FFE), jnp.float32) ** shard_levels(keys[5], (D, FFE), ((0, 8), (1, 4)), -0.2, 0.2)), 0.001, 0.1)
    dense_partial = heavy_noise(keys[6], (N_DP, N_EXPERT, GAINS), 0.1, 0.8, ((0, 8), (1, 4)), (0, 2, 8, 2.0), jnp.float32)
    dense_master = jnp.clip(1.0 + 0.1 * jax.random.normal(keys[7], (GAINS,), jnp.float32), 0.5, 1.5)
    dense_mom = scatter_about(keys[8], (GAINS,), 0.3, 2.0, (), jnp.float32)
    dense_var = jnp.clip(jnp.exp(jax.random.uniform(keys[9], (GAINS,), jnp.float32, math.log(0.1), math.log(10.0))), 0.1, 10.0)
    return {"hidden_act": hidden_act, "out_grad": out_grad, "counts": counts, "expert_master": expert_master, "expert_mom": expert_mom, "expert_var": expert_var, "dense_partial": dense_partial, "dense_master": dense_master, "dense_mom": dense_mom, "dense_var": dense_var}


beta_one = 0.9
beta_two = 0.95
learn_rate = 0.00022
decay_rate = 0.1
epsilon = 1e-08
step_count = 100

def adamw(gradient, master, moment, second):
    moment_new = beta_one * moment + (1.0 - beta_one) * gradient
    second_new = beta_two * second + (1.0 - beta_two) * gradient * gradient
    first_fix = 1.0 - beta_one ** step_count
    second_fix = 1.0 - beta_two ** step_count
    update = moment_new / first_fix / (jnp.sqrt(second_new / second_fix) + epsilon) + decay_rate * master
    return (master - learn_rate * update, moment_new, second_new)

def reference(hidden_act, out_grad, counts, expert_master, expert_mom, expert_var, dense_partial, dense_master, dense_mom, dense_var):
    row_index = jnp.arange(ROWS, dtype=jnp.int32)
    owners = row_index // CAP
    row_live = row_index % CAP < counts[owners]
    masked = jnp.where(row_live[:, None], hidden_act, jnp.zeros_like(hidden_act))
    expert_grad = jnp.dot(out_grad.T, masked, preferred_element_type=jnp.float32)
    dense_grad = lax.optimization_barrier(jnp.sum(dense_partial, axis=(0, 1)))
    master_new, moment_new, second_new = adamw(expert_grad, expert_master, expert_mom, expert_var)
    dense_new, dense_moment, dense_second = adamw(dense_grad, dense_master, dense_mom, dense_var)
    routed_weight = master_new.astype(jnp.bfloat16)
    return (routed_weight, master_new, moment_new, second_new, dense_new, dense_moment, dense_second)
```

```python
import math

import jax
import jax.numpy as jnp
from jax import lax
from jax.experimental.layout import Layout, with_layout_constraint
from jax.sharding import PartitionSpec as P

beta_one = 0.9
beta_two = 0.95
learn_rate = 0.00022
decay_rate = 0.1
epsilon = 1e-08
step_count = 100


def adamw(gradient, master, moment, second):
    moment_new = beta_one * moment + (1.0 - beta_one) * gradient
    second_new = beta_two * second + (1.0 - beta_two) * gradient * gradient
    first_fix = 1.0 - beta_one**step_count
    second_fix = 1.0 - beta_two**step_count
    update = (
        moment_new / first_fix / (jnp.sqrt(second_new / second_fix) + epsilon) + decay_rate * master
    )
    return (master - learn_rate * update, moment_new, second_new)


def swap(value, axis, size, bit):
    return lax.ppermute(value, axis, [(i, i ^ bit) for i in range(size)])


def half(value):
    return value.astype(jnp.float16)


def wide(value):
    return value.astype(jnp.float32)


def tdot(left, right):
    return lax.dot_general(
        left, right, (((0,), (0,)), ((), ())), preferred_element_type=jnp.float32
    )


def is_power(number):
    return number & (number - 1) == 0


def butterfly_sum(value, n_dp, n_expert):
    if not (is_power(n_dp) and is_power(n_expert)):
        return lax.psum(value, ("dp", "expert"))
    bit = n_dp // 2
    while bit:
        value = value + swap(value, "dp", n_dp, bit)
        bit //= 2
    bit = n_expert // 2
    while bit:
        value = value + swap(value, "expert", n_expert, bit)
        bit //= 2
    return value


def make_on_device(n_dp, n_expert):
    chips = n_dp // 2

    def on_device(
        hidden_act,
        out_grad,
        counts,
        expert_master,
        expert_mom,
        expert_var,
        dense_partial,
        dense_master,
        dense_mom,
        dense_var,
    ):
        slots, width = hidden_act.shape
        rows = out_grad.shape[1] // n_dp
        me = lax.axis_index("dp")
        chip, core = me // 2, me % 2
        scale = 2.0 ** math.floor(math.log2(65000.0 / (0.75 * slots * n_dp)))
        row_live = lax.iota(jnp.int32, slots) < counts[0]
        masked = jnp.where(
            row_live[:, None], hidden_act * jnp.asarray(scale, hidden_act.dtype), jnp.zeros_like(hidden_act)
        )

        def block(index):
            return lax.dynamic_slice_in_dim(out_grad, index * rows, rows, 1)

        dense_grad = butterfly_sum(dense_partial.reshape(-1), n_dp, n_expert)
        masked_far = swap(masked, "dp", n_dp, 1)

        def partial(relative):
            target = chip ^ relative
            far = swap(block(2 * target + 1 - core), "dp", n_dp, 1)
            return tdot(masked, block(2 * target + core)) + tdot(masked_far, far)

        if chips == 4:
            cut = width // 2
            part_d = partial(3)
            d_a = swap(half(part_d[:cut]), "dp", n_dp, 2)
            d_b = swap(half(part_d[cut:]), "dp", n_dp, 4)
            part_x = partial(1)
            x_a = swap(half(part_x[:cut]), "dp", n_dp, 2)
            part_y = partial(2)
            y_b = swap(half(part_y[cut:]), "dp", n_dp, 4)
            part_o = partial(0)
            y_a = swap(half(part_y[:cut] + wide(d_a)), "dp", n_dp, 4)
            x_b = swap(half(part_x[cut:] + wide(d_b)), "dp", n_dp, 2)
            grad = jnp.concatenate(
                [
                    part_o[:cut] + wide(x_a) + wide(y_a),
                    part_o[cut:] + wide(y_b) + wide(x_b),
                ],
                axis=0,
            )
        else:
            groups = [[2 * i + k for i in range(chips)] for k in range(2)]
            parts = jnp.stack([half(partial(chip ^ i)) for i in range(chips)])
            grad = wide(
                lax.all_to_all(parts, "dp", 0, 0, axis_index_groups=groups, tiled=True)
            ).sum(axis=0)
        expert_grad = with_layout_constraint(grad.T, Layout((0, 1))) * (1.0 / scale)
        master_new, moment_new, second_new = adamw(
            expert_grad, expert_master, expert_mom, expert_var
        )
        weight = master_new.astype(jnp.bfloat16)
        if chips == 4:
            cut = rows // 2
            w_a, w_b = weight[:cut], weight[cut:]
            ax = swap(w_a, "dp", n_dp, 2)
            by = swap(w_b, "dp", n_dp, 4)
            bx = swap(w_b, "dp", n_dp, 2)
            ay = swap(w_a, "dp", n_dp, 4)
            ad = swap(ax, "dp", n_dp, 4)
            bd = swap(by, "dp", n_dp, 2)
            routed = jnp.zeros((rows * n_dp, width), jnp.bfloat16)
            pieces = [
                (0, 0, w_a), (0, 1, w_b), (1, 0, ax), (2, 1, by),
                (1, 1, bx), (2, 0, ay), (3, 0, ad), (3, 1, bd),
            ]
            for relative, part, piece in pieces:
                base = (chip ^ relative) * 2
                far = swap(piece, "dp", n_dp, 1)
                routed = lax.dynamic_update_slice_in_dim(
                    routed, piece, (base + core) * rows + part * cut, 0
                )
                routed = lax.dynamic_update_slice_in_dim(
                    routed, far, (base + 1 - core) * rows + part * cut, 0
                )
        else:
            routed = lax.all_gather(weight, "dp", axis=0, tiled=True)
        dense_new, dense_moment, dense_second = adamw(
            dense_grad, dense_master, dense_mom, dense_var
        )
        return (
            routed,
            master_new,
            moment_new,
            second_new,
            dense_new,
            dense_moment,
            dense_second,
        )

    return on_device


def solution(mesh):
    in_specs = (
        P("dp", "expert"),
        P("dp", None),
        P("dp"),
        P("dp", "expert"),
        P("dp", "expert"),
        P("dp", "expert"),
        P("dp", "expert", None),
        P(),
        P(),
        P(),
    )
    out_specs = (
        P(None, "expert"),
        P("dp", "expert"),
        P("dp", "expert"),
        P("dp", "expert"),
        P(),
        P(),
        P(),
    )
    return jax.shard_map(
        make_on_device(mesh.shape["dp"], mesh.shape["expert"]),
        mesh=mesh,
        in_specs=in_specs,
        out_specs=out_specs,
        check_vma=False,
    )
```

```python
import math

import jax
import jax.numpy as jnp
from jax import lax
from jax.experimental.layout import Layout, with_layout_constraint
from jax.sharding import PartitionSpec as P

beta_one = 0.9
beta_two = 0.95
learn_rate = 0.00022
decay_rate = 0.1
epsilon = 1e-08
step_count = 100


def adamw(gradient, master, moment, second):
    moment_new = beta_one * moment + (1.0 - beta_one) * gradient
    second_new = beta_two * second + (1.0 - beta_two) * gradient * gradient
    first_fix = 1.0 - beta_one**step_count
    second_fix = 1.0 - beta_two**step_count
    update = (
        moment_new / first_fix / (jnp.sqrt(second_new / second_fix) + epsilon) + decay_rate * master
    )
    return (master - learn_rate * update, moment_new, second_new)


def swap(value, axis, size, bit):
    return lax.ppermute(value, axis, [(i, i ^ bit) for i in range(size)])


def half(value):
    return value.astype(jnp.float16)


def wide(value):
    return value.astype(jnp.float32)


def tdot(left, right):
    return lax.dot_general(
        left, right, (((0,), (0,)), ((), ())), preferred_element_type=jnp.float32
    )


def is_power(number):
    return number & (number - 1) == 0


def butterfly_sum(value, n_dp, n_expert):
    if not (is_power(n_dp) and is_power(n_expert)):
        return lax.psum(value, ("dp", "expert"))
    bit = 1
    while bit < n_expert:
        value = value + swap(value, "expert", n_expert, bit)
        bit *= 2
    bit = 1
    while bit < n_dp:
        value = value + swap(value, "dp", n_dp, bit)
        bit *= 2
    return value


def make_on_device(n_dp, n_expert):
    chips = n_dp // 2

    def on_device(
        hidden_act,
        out_grad,
        counts,
        expert_master,
        expert_mom,
        expert_var,
        dense_partial,
        dense_master,
        dense_mom,
        dense_var,
    ):
        slots, width = hidden_act.shape
        rows = out_grad.shape[1] // n_dp
        me = lax.axis_index("dp")
        chip, core = me // 2, me % 2
        scale = 2.0 ** math.floor(math.log2(65000.0 / (0.75 * slots * n_dp)))
        row_live = lax.iota(jnp.int32, slots) < counts[0]
        masked = jnp.where(
            row_live[:, None], hidden_act * jnp.asarray(scale, hidden_act.dtype), jnp.zeros_like(hidden_act)
        )

        far_core = 1 - core

        def block(source, index, first, count):
            return lax.dynamic_slice_in_dim(source, index * rows + first, count, 1)

        def dense_sum(value, after):
            value, _ = lax.optimization_barrier((value, after))
            return butterfly_sum(value, n_dp, n_expert)

        dense_local = dense_partial.reshape(-1)
        masked_far = swap(masked, "dp", n_dp, 1)

        if chips == 4:
            cut = width // 2
            first_rows = rows * 3 // 7 // 128 * 128
            waves = [(0, rows)]

            def take(source, relative, wave, side):
                return block(source, 2 * (chip ^ relative) + side, *wave)

            def gate(values, after):
                return lax.optimization_barrier((*values, after))[:-1]

            def partial(number, relative, sources):
                near, remote, table = sources
                far = swap(take(table, relative, waves[number], far_core), "dp", n_dp, 1)
                return tdot(near, take(table, relative, waves[number], core)) + tdot(remote, far)

            routed = jnp.zeros((rows * n_dp, width), jnp.bfloat16)
            shards = []
            dense_grad = None
            sources = (masked, masked_far, out_grad)
            for number, (start, count) in enumerate(waves):
                part_d = half(partial(number, 3, sources))
                d_a = swap(part_d[:cut], "dp", n_dp, 2)
                d_b = swap(part_d[cut:], "dp", n_dp, 4)
                sources = gate(sources, part_d)
                part_x = partial(number, 1, sources)
                early_x = half(part_x[:cut])
                x_a = swap(early_x, "dp", n_dp, 2)
                (part_x,) = gate((part_x,), early_x)
                part_y = partial(number, 2, sources)
                early_y = half(part_y[cut:])
                y_b = swap(early_y, "dp", n_dp, 4)
                (part_y,) = gate((part_y,), early_y)
                part_o = partial(number, 0, sources)
                sources = gate(sources, part_o)
                d_a, d_b = gate((d_a, d_b), part_o)
                y_a = swap(half(part_y[:cut] + wide(d_a)), "dp", n_dp, 4)
                sent_x = half(part_x[cut:] + wide(d_b))
                x_b = swap(sent_x, "dp", n_dp, 2)
                if dense_grad is None:
                    dense_grad = dense_sum(dense_local, sent_x)
                grad = jnp.concatenate(
                    [
                        part_o[:cut] + wide(x_a) + wide(y_a),
                        part_o[cut:] + wide(y_b) + wide(x_b),
                    ],
                    axis=0,
                )
                if number == 0:
                    grad, dense_grad = lax.optimization_barrier((grad, dense_grad))
                shard_grad = with_layout_constraint(grad.T, Layout((0, 1))) * (1.0 / scale)
                window = slice(start, start + count)
                shards.append(
                    adamw(
                        shard_grad, expert_master[window], expert_mom[window], expert_var[window]
                    )
                )
            for (start, count), shard in zip(waves, shards):
                weight = shard[0].astype(jnp.bfloat16)
                middle = count // 2
                w_a, w_b = weight[:middle], weight[middle:]
                ax = swap(w_a, "dp", n_dp, 2)
                by = swap(w_b, "dp", n_dp, 4)
                bx = swap(w_b, "dp", n_dp, 2)
                ay = swap(w_a, "dp", n_dp, 4)
                ad = swap(ax, "dp", n_dp, 4)
                bd = swap(by, "dp", n_dp, 2)
                whole = swap(weight, "dp", n_dp, 1)
                routed, _ = lax.optimization_barrier((routed, weight))
                base = chip * 2
                routed = lax.dynamic_update_slice_in_dim(
                    routed, weight, (base + core) * rows + start, 0
                )
                routed = lax.dynamic_update_slice_in_dim(
                    routed, whole, (base + far_core) * rows + start, 0
                )
                for relative, part, piece in (
                    (1, 0, ax), (2, 1, by), (1, 1, bx), (2, 0, ay), (3, 0, ad), (3, 1, bd)
                ):
                    base = (chip ^ relative) * 2
                    place = start + part * middle
                    other = swap(piece, "dp", n_dp, 1)
                    routed = lax.dynamic_update_slice_in_dim(
                        routed, piece, (base + core) * rows + place, 0
                    )
                    routed = lax.dynamic_update_slice_in_dim(
                        routed, other, (base + far_core) * rows + place, 0
                    )
            master_new, moment_new, second_new = (
                jnp.concatenate(parts, axis=0) for parts in zip(*shards)
            )
        else:
            groups = [[2 * i + k for i in range(chips)] for k in range(2)]

            def partial(target):
                other = swap(
                    block(out_grad, 2 * target + far_core, 0, rows), "dp", n_dp, 1
                )
                return tdot(masked, block(out_grad, 2 * target + core, 0, rows)) + tdot(
                    masked_far, other
                )

            parts = jnp.stack([half(partial(i)) for i in range(chips)])
            grad = wide(
                lax.all_to_all(parts, "dp", 0, 0, axis_index_groups=groups, tiled=True)
            ).sum(axis=0)
            master_new, moment_new, second_new = adamw(
                grad.T * (1.0 / scale), expert_master, expert_mom, expert_var
            )
            routed = lax.all_gather(master_new.astype(jnp.bfloat16), "dp", axis=0, tiled=True)
            dense_grad = butterfly_sum(dense_local, n_dp, n_expert)
        dense_new, dense_moment, dense_second = adamw(
            dense_grad, dense_master, dense_mom, dense_var
        )
        return (
            routed,
            master_new,
            moment_new,
            second_new,
            dense_new,
            dense_moment,
            dense_second,
        )

    return on_device


def solution(mesh):
    in_specs = (
        P("dp", "expert"),
        P("dp", None),
        P("dp"),
        P("dp", "expert"),
        P("dp", "expert"),
        P("dp", "expert"),
        P("dp", "expert", None),
        P(),
        P(),
        P(),
    )
    out_specs = (
        P(None, "expert"),
        P("dp", "expert"),
        P("dp", "expert"),
        P("dp", "expert"),
        P(),
        P(),
        P(),
    )
    return jax.shard_map(
        make_on_device(mesh.shape["dp"], mesh.shape["expert"]),
        mesh=mesh,
        in_specs=in_specs,
        out_specs=out_specs,
        check_vma=False,
    )
```
